32 devices in a mesh: patch: 32 (over z, y, x, core).
Axes of the slice: x: 2, y: 2, z: 4, core: 2. Of those that a mesh axis runs over, the one named last changes fastest.
Arguments:
- atm_flux: bfloat16 [8, 98304], P(None, 'patch'), may hold values from -6 to 6
- remap_send: int32 [32, 5, 8], P('patch'), may hold values from 0 to 23
- remap_target: int32 [32, 5, 8], P('patch'), may hold values from 0 to 31
- remap_counts: int32 [32, 5], P('patch'), may hold values from 0 to 8, as said below
- remap_weights: bfloat16 [32, 5, 8, 128, 128], P('patch'), may hold values from -0.5 to 0.5
- coupling: float32 [2, 8], replicated, may hold values from -2 to 2
- tracer: float32 [2, 128, 131072], P(None, None, 'patch'), may hold values from -6 to 6
- wet: int32 [131072], P('patch'), may hold values from 0 to 1
- mix_inverse: float32 [1024, 128, 128], P('patch')
- halo_send: int32 [32, 4, 2, 128], P('patch'), may hold values from 0 to 4095
- halo_ghost: int32 [32, 4, 2, 128], P('patch'), may hold values from 0 to 4095
- halo_rows: int32 [32, 4], P('patch'), may hold values from 0 to 2, as said below
Outputs:
- ocean_flux: float32 [8, 131072], P(None, 'patch')
- tracer_out: float32 [2, 128, 131072], P(None, None, 'patch')
The draws below stay inside these ranges and needn't reach their ends.
Inputs may be any that keep to these rules, and one draw needn't show every extreme that they name: `remap_counts`: some entry equals 8. `halo_rows`: some entry equals 2.
All inputs are finite; a program needn't handle non-finite values.
Results may differ from the reference program's by a relative error of at most 0.0003.
Values may be sent and summed in bfloat16 or wider, within the bound.
A program may use at most 64 MiB of HBM per device.

```python
import math
import jax
import jax.numpy as jnp
from jax import lax

F = 8
LEV = 128
NTR = 2
BLOCK = 128
ABLK = 24
OBLK = 32
CAP = 8
REACH = 2
HR = 2
SPAN = 5
HSPAN = 4
OC = 4096
NOC = 131072
NA = 98304
N_PATCH = 32


def force_top(key, rows, columns, top):
    counts = jax.random.randint(jax.random.fold_in(key, 21), (rows * columns,), 0, top + 1)
    spot = jax.random.randint(jax.random.fold_in(key, 22), (), 0, rows * columns)
    counts = jnp.where(jnp.arange(rows * columns) == spot, top, counts)
    return counts.reshape(rows, columns).astype(jnp.int32)


def draw_remap_counts(key, part):
    return force_top(jax.random.fold_in(key, 31), N_PATCH, SPAN, CAP)


def draw_halo_rows(key, part):
    return force_top(jax.random.fold_in(key, 41), N_PATCH, HSPAN, HR)


def draw_wet(key, part):
    percent = jax.random.randint(jax.random.fold_in(key, 51), (N_PATCH, 1), 30, 96)
    rolled = jax.random.randint(jax.random.fold_in(key, 52), (N_PATCH, OBLK * BLOCK), 0, 100)
    return (rolled < percent).astype(jnp.int32).reshape(-1)


def draw_mix_inverse(key, part):
    count = N_PATCH * OBLK
    diag = jax.random.uniform(jax.random.fold_in(key, 61), (count, LEV, 1), jnp.float32, 0.6, 1.4)
    eye = jnp.eye(LEV, dtype=jnp.float32)[None, :, :]
    spread = 0.5 * jax.random.normal(jax.random.fold_in(key, 63), (count, LEV, LEV), jnp.float32)
    return (eye * diag + spread / math.sqrt(LEV)).astype(jnp.float32)


def plant(values, stream_key, low, largest):
    longest = values.shape.index(max(values.shape))
    spots = []
    for shift in (0, 1):
        where = [jax.random.randint(jax.random.fold_in(stream_key, axis), (), 0, length) for axis, length in enumerate(values.shape)]
        where[longest] = (where[longest] + shift) % values.shape[longest]
        spots.append(tuple(where))
    return values.at[spots[0]].set(low).at[spots[1]].set(largest)


def block_scale(own_key, extent, cuts, low, largest):
    loudness = 1.0
    for axis_at, shards_of in cuts:
        draws = jax.random.uniform(jax.random.fold_in(jax.random.fold_in(own_key, 6), axis_at), (shards_of,), jnp.float32, low / len(cuts), largest / len(cuts))
        loudness = loudness * jnp.repeat(jnp.exp(draws), extent[axis_at] // shards_of).reshape((-1,) + (1,) * (len(extent) - 1 - axis_at))
    return loudness


def centred(rng, shape, width, limit, split=(), kind=jnp.bfloat16):
    gain = block_scale(rng, shape, split, -0.22, 0.18) if split else 1.0
    drawn = jax.random.normal(rng, shape, jnp.float32) * width * gain
    return jnp.minimum(jnp.maximum(drawn, -limit), limit).astype(kind)


def setup_inputs(seed: int = 0) -> dict:
    key_of = jax.random.split(jax.random.key(seed), 13)
    atm_flux = centred(key_of[0], (F, NA), 1.0, 6.0, ((1, 32),))
    remap_send = plant(jax.random.randint(key_of[1], (N_PATCH, SPAN, CAP), 0, ABLK), jax.random.fold_in(key_of[1], 1), 0, ABLK - 1).astype(jnp.int32)
    remap_target = plant(jax.random.randint(key_of[2], (N_PATCH, SPAN, CAP), 0, OBLK), jax.random.fold_in(key_of[2], 1), 0, OBLK - 1).astype(jnp.int32)
    remap_counts = draw_remap_counts(jax.random.fold_in(key_of[12], 71), 0)
    remap_weights = centred(key_of[4], (N_PATCH, SPAN, CAP, BLOCK, BLOCK), BLOCK ** -0.5, 0.5, ((0, 32),))
    coupling = centred(key_of[5], (NTR, F), F ** -0.5, 2.0, (), jnp.float32)
    tracer = centred(key_of[6], (NTR, LEV, NOC), 1.0, 6.0, ((2, 32),), jnp.float32)
    wet = draw_wet(jax.random.fold_in(key_of[12], 71), 0)
    mix_inverse = draw_mix_inverse(jax.random.fold_in(key_of[12], 71), 0)
    halo_send = plant(jax.random.randint(key_of[9], (N_PATCH, HSPAN, HR, BLOCK), 0, OC), jax.random.fold_in(key_of[9], 1), 0, OC - 1).astype(jnp.int32)
    halo_ghost = plant(jax.random.randint(key_of[10], (N_PATCH, HSPAN, HR, BLOCK), 0, OC), jax.random.fold_in(key_of[10], 1), 0, OC - 1).astype(jnp.int32)
    halo_rows = draw_halo_rows(jax.random.fold_in(key_of[12], 71), 0)
    return dict(atm_flux=atm_flux, remap_send=remap_send, remap_target=remap_target, remap_counts=remap_counts, remap_weights=remap_weights, coupling=coupling, tracer=tracer, wet=wet, mix_inverse=mix_inverse, halo_send=halo_send, halo_ghost=halo_ghost, halo_rows=halo_rows)


def reference(atm_flux, remap_send, remap_target, remap_counts, remap_weights, coupling, tracer, wet, mix_inverse, halo_send, halo_ghost, halo_rows):
    wetf = wet.astype(jnp.float32)
    offsets = jnp.arange(SPAN, dtype=jnp.int32) - REACH
    blocks = atm_flux.reshape(F, N_PATCH * ABLK, BLOCK)

    def receive(ocean):
        source = (ocean - offsets) % N_PATCH
        global_id = source[:, None] * ABLK + remap_send[source, jnp.arange(SPAN, dtype=jnp.int32)]
        pieces = blocks[:, global_id].astype(jnp.float32)
        in_use = (jnp.arange(CAP, dtype=jnp.int32)[None, :] < remap_counts[ocean][:, None]).astype(jnp.float32)
        contrib = jnp.einsum("fdci,dcij->dcfj", pieces, remap_weights[ocean].astype(jnp.float32), precision=lax.Precision.HIGHEST)
        contrib = contrib * in_use[:, :, None, None]
        table = (remap_target[ocean][..., None] == jnp.arange(OBLK, dtype=jnp.int32)).astype(jnp.float32)
        return jnp.einsum("dcb,dcfj->fbj", table, contrib, precision=lax.Precision.HIGHEST).reshape(F, OBLK * BLOCK)

    flux = lax.map(receive, jnp.arange(N_PATCH, dtype=jnp.int32))
    ocean_flux = jnp.transpose(flux, (1, 0, 2)).reshape(F, NOC) * wetf
    surface = jnp.dot(coupling, ocean_flux, precision=lax.Precision.HIGHEST)
    rhs = tracer.at[:, 0, :].add(surface)
    shaped = rhs.reshape(NTR, LEV, N_PATCH * OBLK, BLOCK)
    solved = jnp.einsum("blk,tkbc->tlbc", mix_inverse, shaped, precision=lax.Precision.HIGHEST).reshape(NTR, LEV, NOC)
    mixed = wetf * solved + (1.0 - wetf) * tracer
    sent = mixed.astype(jnp.bfloat16)
    halo_offsets = jnp.concatenate([jnp.arange(-REACH, 0, dtype=jnp.int32), jnp.arange(1, REACH + 1, dtype=jnp.int32)])
    ocean_ids = jnp.arange(N_PATCH, dtype=jnp.int32)[:, None]
    source = (ocean_ids - halo_offsets[None, :]) % N_PATCH
    source_cells = halo_send[source, jnp.arange(HSPAN, dtype=jnp.int32)[None, :]]
    source_glob = source[:, :, None, None] * OC + source_cells
    target_glob = ocean_ids[:, :, None, None] * OC + halo_ghost
    in_use = (jnp.arange(HR, dtype=jnp.int32)[None, None, :] < halo_rows[:, :, None]).astype(jnp.float32)
    values = sent[:, :, source_glob].astype(jnp.float32)
    current = mixed[:, :, target_glob]
    weight = in_use[..., None] * wetf[target_glob]
    increment = 0.25 * (values - current) * weight
    tracer_out = mixed.at[:, :, target_glob].add(increment)
    return ocean_flux, tracer_out
```

```python
import jax
import jax.numpy as jnp
from jax import lax
from jax.sharding import PartitionSpec as P


def shifted(array, axis, by):
    length = lax.axis_size(axis)
    return lax.ppermute(array, axis, [(i, (i + by) % length) for i in range(length)])


def route_fluxes(outgoing, offsets):
    pieces = [shifted(outgoing[index], "patch", offsets[index]) for index in range(len(offsets))]
    return jnp.stack(pieces)


def route_halo(outgoing, offsets):
    pieces = [shifted(outgoing[index], "patch", offsets[index]) for index in range(len(offsets))]
    return jnp.stack(pieces)


def body(
    atm_flux,
    remap_send,
    remap_target,
    remap_counts,
    remap_weights,
    coupling,
    tracer,
    wet,
    mix_inverse,
    halo_send,
    halo_ghost,
    halo_rows,
):
    offset_count = remap_send.shape[1]
    radius = offset_count // 2
    capacity = remap_send.shape[2]
    block_cells = remap_weights.shape[-1]
    flux_count = atm_flux.shape[0]
    tracers, levels, ocean_cells = tracer.shape
    ocean_blocks = ocean_cells // block_cells
    atm_blocks = atm_flux.shape[1] // block_cells
    wetf = wet.astype(jnp.float32)
    blocks = atm_flux.reshape(flux_count, atm_blocks, block_cells)
    chooser = (
        remap_send[0].reshape(-1)[:, None] == jnp.arange(atm_blocks, dtype=jnp.int32)[None, :]
    ).astype(jnp.bfloat16)
    selected = jnp.einsum(
        "sa,fab->sfb", chooser, blocks, preferred_element_type=jnp.float32
    ).astype(jnp.bfloat16)
    outgoing = selected.reshape(offset_count, capacity, flux_count, block_cells)
    flux_offsets = [index - radius for index in range(offset_count)]
    arrived = route_fluxes(outgoing, flux_offsets)
    in_use = (jnp.arange(capacity, dtype=jnp.int32)[None, :] < remap_counts[0][:, None]).astype(
        jnp.float32
    )
    contrib = jnp.einsum(
        "dcfi,dcij->dcfj", arrived, remap_weights[0], preferred_element_type=jnp.float32
    )
    contrib = contrib * in_use[:, :, None, None]
    table = (remap_target[0][..., None] == jnp.arange(ocean_blocks, dtype=jnp.int32)).astype(
        jnp.float32
    )
    ocean_flux = (
        jnp.einsum("dcb,dcfj->fbj", table, contrib, precision=lax.Precision.HIGHEST).reshape(
            flux_count, ocean_cells
        )
        * wetf
    )
    surface = jnp.dot(coupling, ocean_flux, precision=lax.Precision.HIGHEST)
    rhs = jnp.concatenate([tracer[:, 0:1, :] + surface[:, None, :], tracer[:, 1:, :]], axis=1)
    shaped = rhs.reshape(tracers, levels, ocean_blocks, block_cells)
    solved = jnp.einsum(
        "blk,tkbc->tlbc", mix_inverse, shaped, precision=lax.Precision.HIGH
    ).reshape(tracers, levels, ocean_cells)
    mixed = wetf * solved + (1.0 - wetf) * tracer
    sent = mixed.astype(jnp.bfloat16)
    halo_count = halo_send.shape[1]
    halo_depth = halo_send.shape[2]
    lanes = halo_send.shape[3]
    picks = halo_count * halo_depth * lanes
    cell_ids = jnp.arange(ocean_cells, dtype=jnp.int32)
    source_table = (cell_ids[:, None] == halo_send[0].reshape(-1)[None, :]).astype(jnp.bfloat16)
    gathered = jnp.dot(
        sent.reshape(tracers * levels, ocean_cells),
        source_table,
        preferred_element_type=jnp.float32,
    ).astype(jnp.bfloat16)
    gathered = gathered.reshape(tracers, levels, halo_count, halo_depth, lanes)
    halo_offsets = [index - radius for index in range(radius)] + [
        index + 1 for index in range(radius)
    ]
    halo_out = jnp.transpose(gathered, (2, 3, 0, 1, 4))
    received = route_halo(halo_out, halo_offsets)
    values = (
        jnp.transpose(received, (2, 3, 0, 1, 4))
        .reshape(tracers * levels, picks)
    )
    rows_used = jnp.arange(halo_depth, dtype=jnp.int32)[None, :] < halo_rows[0][:, None]
    used = jnp.broadcast_to(rows_used[:, :, None], (halo_count, halo_depth, lanes)).reshape(-1)
    ghost_table = (
        (halo_ghost[0].reshape(-1)[:, None] == cell_ids[None, :]) & used[:, None]
    ).astype(jnp.bfloat16)
    flat_mixed = mixed.reshape(tracers * levels, ocean_cells)
    summed = jnp.dot(values, ghost_table, preferred_element_type=jnp.float32)
    hits = jnp.sum(ghost_table.astype(jnp.float32), axis=0)
    pull = 0.25 * wetf
    tracer_out = (flat_mixed + pull[None, :] * (summed - hits[None, :] * flat_mixed)).reshape(
        tracers, levels, ocean_cells
    )
    return (ocean_flux, tracer_out)


def solution(mesh):
    return jax.shard_map(
        body,
        mesh=mesh,
        in_specs=(
            P(None, "patch"),
            P("patch", None, None),
            P("patch", None, None),
            P("patch", None),
            P("patch", None, None, None, None),
            P(),
            P(None, None, "patch"),
            P("patch"),
            P("patch", None, None),
            P("patch", None, None, None),
            P("patch", None, None, None),
            P("patch", None),
        ),
        out_specs=(P(None, "patch"), P(None, None, "patch")),
        check_vma=False,
    )
```

```python
import jax
import jax.numpy as jnp
from jax import lax
from jax.experimental import pallas as pl
from jax.experimental.pallas import tpu as pltpu
from jax.sharding import PartitionSpec as P

MESH = pl.DeviceIdType.MESH
CHUNKS = 8
TILE = 1024


def split(value):
    high = value.astype(jnp.bfloat16)
    return high, (value - high.astype(jnp.float32)).astype(jnp.bfloat16)


def product(left, right):
    return jnp.dot(left, right, preferred_element_type=jnp.float32)


def couple_kernel(
    remap_send,
    remap_target,
    remap_counts,
    coupling,
    atm,
    wet,
    halo_send,
    weights_hbm,
    tracer_hbm,
    inverse_hbm,
    flux_out,
    mixed,
    received,
    weights,
    tracer,
    inverse,
    sent,
    surface,
    total,
    outgoing,
    arrived,
    tables,
    picked,
    load_sem,
    flux_send_sem,
    flux_recv_sem,
    halo_send_sem,
    halo_recv_sem,
):
    size = lax.axis_size("patch")
    me = lax.axis_index("patch")
    spans, slots = remap_send.shape[1], remap_send.shape[2]
    radius = spans // 2
    tracers, levels, cells = tracer.shape
    block = weights.shape[-1]
    blocks = cells // block
    fluxes = atm.shape[0]
    steps = [d - radius for d in range(spans) if d != radius]
    depth, lanes = halo_send.shape[2], halo_send.shape[3]

    def peer(step):
        return lax.rem(me + step + size, size)

    weight_load = pltpu.make_async_copy(weights_hbm.at[0], weights, load_sem.at[2 * CHUNKS])
    weight_load.start()
    part, span = blocks // CHUNKS, cells // CHUNKS
    loads = []
    for chunk in range(CHUNKS):
        run = pl.ds(chunk * span, span)
        loads.append(
            pltpu.make_async_copy(
                tracer_hbm.at[:, :, run], tracer.at[:, :, run], load_sem.at[2 * chunk]
            )
        )
        group = pl.ds(chunk * part, part)
        loads.append(
            pltpu.make_async_copy(
                inverse_hbm.at[group], inverse.at[group], load_sem.at[2 * chunk + 1]
            )
        )
    for load in loads:
        load.start()

    barrier = pltpu.get_barrier_semaphore()
    for step in steps:
        pl.semaphore_signal(barrier, inc=1, device_id=(peer(step),), device_id_type=MESH)
    sources = [
        atm[:, a * block : (a + 1) * block].astype(jnp.float32)
        for a in range(atm.shape[1] // block)
    ]
    blank = jnp.zeros((fluxes, block), jnp.int32)
    for d in range(spans):
        for c in range(slots):
            wanted = blank + remap_send[0, d, c]
            piece = sources[0]
            for a in range(1, len(sources)):
                piece = jnp.where(wanted == a, sources[a], piece)
            piece = piece.astype(jnp.bfloat16)
            if d == radius:
                arrived[d, c] = piece
            else:
                outgoing[d, c] = piece
    pl.semaphore_wait(barrier, len(steps))
    flux_copies = []
    for d in range(spans):
        if d == radius:
            continue
        copy = pltpu.make_async_remote_copy(
            src_ref=outgoing.at[d],
            dst_ref=arrived.at[d],
            send_sem=flux_send_sem.at[d],
            recv_sem=flux_recv_sem.at[d],
            device_id=(peer(d - radius),),
            device_id_type=MESH,
        )
        copy.start()
        flux_copies.append(copy)

    rows = 512

    def table_rows(index, _):
        base = pl.multiple_of(index * rows, rows)
        ids = lax.broadcasted_iota(jnp.int32, (rows, lanes), 0) + base
        for h in range(len(steps)):
            for r in range(depth):
                hit = ids == halo_send[0, h, r : r + 1, :]
                tables[h, pl.ds(base, rows), r * lanes : (r + 1) * lanes] = jnp.where(
                    hit, 1.0, 0.0
                ).astype(jnp.bfloat16)
        return 0

    lax.fori_loop(0, cells // rows, table_rows, 0)

    weight_load.wait()
    for copy in flux_copies:
        copy.wait()
    owner = lax.broadcasted_iota(jnp.int32, (blocks, fluxes, block), 0)
    for d in range(spans):
        pieces = []
        for c in range(slots):
            used = (blank + remap_counts[0, d]) > c
            piece = jnp.where(used, arrived[d, c].astype(jnp.float32), 0.0)
            placed = jnp.where(owner == remap_target[0, d, c], piece[None], 0.0)
            pieces.append(placed.reshape(blocks * fluxes, block).astype(jnp.bfloat16))
        left = jnp.concatenate(pieces, axis=1)
        term = product(left, weights[d].reshape(slots * block, block))
        if d == 0:
            total[...] = term
        else:
            total[...] += term
    for b in range(blocks):
        run = slice(b * block, (b + 1) * block)
        flux = total[b * fluxes : (b + 1) * fluxes, :] * wet[0:1, run].astype(jnp.float32)
        flux_out[:, run] = flux
        for t in range(tracers):
            value = coupling[t, 0] * flux[0:1, :]
            for f in range(1, fluxes):
                value = value + coupling[t, f] * flux[f : f + 1, :]
            surface[t : t + 1, run] = value

    top = lax.broadcasted_iota(jnp.int32, (levels, block), 0) == 0

    def mix_block(k, _):
        run = pl.ds(pl.multiple_of(k * block, block), block)
        high, low = split(inverse[k])
        wetf = wet[0:1, run].astype(jnp.float32)
        held = [tracer[t, :, run] for t in range(tracers)]
        right = jnp.concatenate(
            [
                held[t] + jnp.where(top, surface[t : t + 1, run], 0.0)
                for t in range(tracers)
            ],
            axis=1,
        )
        right_high, right_low = split(right)
        solved = (
            product(high, right_high) + product(high, right_low) + product(low, right_high)
        )
        for t in range(tracers):
            value = wetf * solved[:, t * block : (t + 1) * block] + (1.0 - wetf) * held[t]
            mixed[t, :, run] = value
            sent[t * levels : (t + 1) * levels, run] = value.astype(jnp.bfloat16)
        return 0

    for chunk in range(CHUNKS):
        loads[2 * chunk].wait()
        loads[2 * chunk + 1].wait()
        lax.fori_loop(chunk * part, (chunk + 1) * part, mix_block, 0)

    order = sorted(range(len(steps)), key=lambda h: (-abs(steps[h]), h))
    halo_copies = []
    for h in order:
        picked[h] = product(sent[...], tables[h]).astype(jnp.bfloat16)
        copy = pltpu.make_async_remote_copy(
            src_ref=picked.at[h],
            dst_ref=received.at[h],
            send_sem=halo_send_sem.at[h],
            recv_sem=halo_recv_sem.at[h],
            device_id=(peer(steps[h]),),
            device_id_type=MESH,
        )
        copy.start()
        halo_copies.append(copy)
    for copy in halo_copies:
        copy.wait()


def halo_kernel(halo_rows, halo_ghost, wet, received, flux_in, mixed, flux_out, out):
    tracers, levels, tile = out.shape
    run = pl.ds(pl.multiple_of(pl.program_id(0) * tile, tile), tile)
    hosts, depth, lanes = halo_ghost.shape[1:]
    ids = lax.broadcasted_iota(jnp.int32, (tile, lanes), 0) + pl.program_id(0) * tile
    columns = []
    for h in range(hosts):
        for r in range(depth):
            ghost = jnp.where(r < halo_rows[0, h], halo_ghost[0, h, r : r + 1, :], -1)
            columns.append(jnp.where(ids == ghost, 1.0, 0.0).astype(jnp.bfloat16))
    table = jnp.concatenate(columns, axis=1)
    values = jnp.concatenate([received[h] for h in range(hosts)], axis=1)
    contract = (((1,), (1,)), ((), ()))
    summed = lax.dot_general(values, table, contract, preferred_element_type=jnp.float32)
    ones = jnp.ones((16, table.shape[1]), jnp.bfloat16)
    hits = lax.dot_general(ones, table, contract, preferred_element_type=jnp.float32)[0:1]
    pull = 0.25 * wet[...].astype(jnp.float32)
    for t in range(tracers):
        value = mixed[t, :, run]
        out[t] = value + pull * (summed[t * levels : (t + 1) * levels] - hits * value)
    flux_out[...] = flux_in[...]


def body(
    atm_flux,
    remap_send,
    remap_target,
    remap_counts,
    remap_weights,
    coupling,
    tracer,
    wet,
    mix_inverse,
    halo_send,
    halo_ghost,
    halo_rows,
):
    spans, slots = remap_send.shape[1:]
    block = remap_weights.shape[-1]
    fluxes = atm_flux.shape[0]
    tracers, levels, cells = tracer.shape
    blocks = cells // block
    hosts, depth, lanes = halo_send.shape[1:]
    picks = depth * lanes
    features = tracers * levels
    wet_row = wet.reshape(1, cells)
    vmem = pl.BlockSpec(memory_space=pltpu.VMEM)
    smem = pl.BlockSpec(memory_space=pltpu.SMEM)
    hbm = pl.BlockSpec(memory_space=pltpu.HBM)
    flux, mixed, received = pl.pallas_call(
        couple_kernel,
        out_shape=(
            pltpu.VMEM((fluxes, cells), jnp.float32),
            pltpu.VMEM((tracers, levels, cells), jnp.float32),
            pltpu.VMEM((hosts, features, picks), jnp.bfloat16),
        ),
        in_specs=[smem] * 4 + [vmem] * 3 + [hbm] * 3,
        out_specs=(vmem, vmem, vmem),
        scratch_shapes=[
            pltpu.VMEM((spans, slots, block, block), jnp.bfloat16),
            pltpu.VMEM((tracers, levels, cells), jnp.float32),
            pltpu.VMEM((blocks, levels, levels), jnp.float32),
            pltpu.VMEM((features, cells), jnp.bfloat16),
            pltpu.VMEM((tracers, cells), jnp.float32),
            pltpu.VMEM((blocks * fluxes, block), jnp.float32),
            pltpu.VMEM((spans, slots, fluxes, block), jnp.bfloat16),
            pltpu.VMEM((spans, slots, fluxes, block), jnp.bfloat16),
            pltpu.VMEM((hosts, cells, picks), jnp.bfloat16),
            pltpu.VMEM((hosts, features, picks), jnp.bfloat16),
            pltpu.SemaphoreType.DMA((2 * CHUNKS + 1,)),
            pltpu.SemaphoreType.DMA((spans,)),
            pltpu.SemaphoreType.DMA((spans,)),
            pltpu.SemaphoreType.DMA((hosts,)),
            pltpu.SemaphoreType.DMA((hosts,)),
        ],
        compiler_params=pltpu.CompilerParams(
            collective_id=0, has_side_effects=True, vmem_limit_bytes=58 * 1024 * 1024
        ),
        name="couple",
    )(
        remap_send,
        remap_target,
        remap_counts,
        coupling,
        atm_flux,
        wet_row,
        halo_send,
        remap_weights,
        tracer,
        mix_inverse,
    )
    tile = min(TILE, cells)
    return pl.pallas_call(
        halo_kernel,
        grid=(cells // tile,),
        out_shape=(
            jax.ShapeDtypeStruct((fluxes, cells), jnp.float32),
            jax.ShapeDtypeStruct((tracers, levels, cells), jnp.float32),
        ),
        in_specs=[
            smem,
            pl.BlockSpec(memory_space=pltpu.VMEM),
            pl.BlockSpec((1, tile), lambda i: (0, i)),
            pl.BlockSpec(memory_space=pltpu.VMEM),
            pl.BlockSpec((fluxes, tile), lambda i: (0, i)),
            pl.BlockSpec(memory_space=pltpu.VMEM),
        ],
        out_specs=(
            pl.BlockSpec((fluxes, tile), lambda i: (0, i)),
            pl.BlockSpec((tracers, levels, tile), lambda i: (0, 0, i)),
        ),
        compiler_params=pltpu.CompilerParams(vmem_limit_bytes=32 * 1024 * 1024),
        name="halo",
    )(halo_rows, halo_ghost, wet_row, received, flux, mixed)


def solution(mesh):
    return jax.shard_map(
        body,
        mesh=mesh,
        in_specs=(
            P(None, "patch"),
            P("patch", None, None),
            P("patch", None, None),
            P("patch", None),
            P("patch", None, None, None, None),
            P(),
            P(None, None, "patch"),
            P("patch"),
            P("patch", None, None),
            P("patch", None, None, None),
            P("patch", None, None, None),
            P("patch", None),
        ),
        out_specs=(P(None, "patch"), P(None, None, "patch")),
        check_vma=False,
    )
```

```python
import jax
import jax.numpy as jnp
from jax import lax
from jax.experimental import pallas as pl
from jax.experimental.pallas import tpu as pltpu
from jax.sharding import PartitionSpec as P

MESH = pl.DeviceIdType.MESH
CHUNKS = 8
TILE = 512


def split(value):
    high = value.astype(jnp.bfloat16)
    return high, (value - high.astype(jnp.float32)).astype(jnp.bfloat16)


def product(left, right):
    return jnp.dot(left, right, preferred_element_type=jnp.float32)


def couple_kernel(
    remap_send,
    remap_target,
    remap_counts,
    coupling,
    halo_rows,
    atm,
    wet,
    halo_send,
    halo_ghost,
    weights_hbm,
    tracer_hbm,
    inverse_hbm,
    flux_out,
    mixed,
    received,
    scatter,
    weights,
    tracer,
    inverse,
    sent,
    surface,
    total,
    outgoing,
    arrived,
    tables,
    picked,
    load_sem,
    flux_send_sem,
    flux_recv_sem,
    halo_send_sem,
    halo_recv_sem,
):
    size = lax.axis_size("patch")
    me = lax.axis_index("patch")
    spans, slots = remap_send.shape[0], remap_send.shape[2]
    radius = spans // 2
    tracers, levels, cells = tracer.shape
    block = weights.shape[-1]
    blocks = cells // block
    fluxes = atm.shape[0]
    steps = [d - radius for d in range(spans) if d != radius]
    depth, lanes = halo_send.shape[2], halo_send.shape[3]

    def peer(step):
        return lax.rem(me + step + size, size)

    weight_load = pltpu.make_async_copy(weights_hbm.at[0], weights, load_sem.at[2 * CHUNKS])
    weight_load.start()
    part, span = blocks // CHUNKS, cells // CHUNKS
    loads = []
    for chunk in range(CHUNKS):
        run = pl.ds(chunk * span, span)
        loads.append(
            pltpu.make_async_copy(
                tracer_hbm.at[:, :, run], tracer.at[:, :, run], load_sem.at[2 * chunk]
            )
        )
        group = pl.ds(chunk * part, part)
        loads.append(
            pltpu.make_async_copy(
                inverse_hbm.at[group], inverse.at[group], load_sem.at[2 * chunk + 1]
            )
        )
    for load in loads:
        load.start()

    barrier = pltpu.get_barrier_semaphore()
    for step in steps:
        pl.semaphore_signal(barrier, inc=1, device_id=(peer(step),), device_id_type=MESH)
    sources = [
        atm[:, a * block : (a + 1) * block].astype(jnp.float32)
        for a in range(atm.shape[1] // block)
    ]
    blank = jnp.zeros((fluxes, block), jnp.int32)
    for d in range(spans):
        for c in range(slots):
            wanted = blank + remap_send[d, 0, c]
            piece = sources[0]
            for a in range(1, len(sources)):
                piece = jnp.where(wanted == a, sources[a], piece)
            piece = piece.astype(jnp.bfloat16)
            if d == radius:
                arrived[d, c] = piece
            else:
                outgoing[d, c] = piece
    pl.semaphore_wait(barrier, len(steps))
    flux_copies = []
    for d in range(spans):
        if d == radius:
            continue
        copy = pltpu.make_async_remote_copy(
            src_ref=outgoing.at[d],
            dst_ref=arrived.at[d],
            send_sem=flux_send_sem.at[d],
            recv_sem=flux_recv_sem.at[d],
            device_id=(peer(d - radius),),
            device_id_type=MESH,
        )
        copy.start()
        flux_copies.append(copy)

    rows = 512

    def table_rows(index, _):
        base = pl.multiple_of(index * rows, rows)
        ids = lax.broadcasted_iota(jnp.int32, (rows, lanes), 0) + base
        for h in range(len(steps)):
            for r in range(depth):
                hit = ids == halo_send[0, h, r : r + 1, :]
                tables[h, pl.ds(base, rows), r * lanes : (r + 1) * lanes] = jnp.where(
                    hit, 1.0, 0.0
                ).astype(jnp.bfloat16)
        return 0

    lax.fori_loop(0, cells // rows, table_rows, 0)

    weight_load.wait()
    for copy in flux_copies:
        copy.wait()
    owner = lax.broadcasted_iota(jnp.int32, (blocks, fluxes, block), 0)
    for d in range(spans):
        pieces = []
        for c in range(slots):
            used = (blank + remap_counts[0, d]) > c
            piece = jnp.where(used, arrived[d, c].astype(jnp.float32), 0.0)
            placed = jnp.where(owner == remap_target[d, 0, c], piece[None], 0.0)
            pieces.append(placed.reshape(blocks * fluxes, block).astype(jnp.bfloat16))
        left = jnp.concatenate(pieces, axis=1)
        term = product(left, weights[d].reshape(slots * block, block))
        if d == 0:
            total[...] = term
        else:
            total[...] += term
    for b in range(blocks):
        run = slice(b * block, (b + 1) * block)
        flux = total[b * fluxes : (b + 1) * fluxes, :] * wet[0:1, run].astype(jnp.float32)
        flux_out[:, run] = flux
        for t in range(tracers):
            value = coupling[t, 0] * flux[0:1, :]
            for f in range(1, fluxes):
                value = value + coupling[t, f] * flux[f : f + 1, :]
            surface[t : t + 1, run] = value

    top = lax.broadcasted_iota(jnp.int32, (levels, block), 0) == 0

    def mix_block(k):
        run = slice(k * block, (k + 1) * block)
        high, low = split(inverse[k])
        wetf = wet[0:1, run].astype(jnp.float32)
        held = [tracer[t, :, run] for t in range(tracers)]
        right = jnp.concatenate(
            [
                held[t] + jnp.where(top, surface[t : t + 1, run], 0.0)
                for t in range(tracers)
            ],
            axis=1,
        )
        right_high, right_low = split(right)
        solved = (
            product(high, right_high) + product(high, right_low) + product(low, right_high)
        )
        for t in range(tracers):
            value = wetf * solved[:, t * block : (t + 1) * block] + (1.0 - wetf) * held[t]
            mixed[t, :, run] = value
            sent[t * levels : (t + 1) * levels, run] = value.astype(jnp.bfloat16)

    for chunk in range(CHUNKS):
        loads[2 * chunk].wait()
        loads[2 * chunk + 1].wait()
        for k in range(chunk * part, (chunk + 1) * part):
            mix_block(k)

    order = sorted(range(len(steps)), key=lambda h: (-abs(steps[h]), h))
    halo_copies = []
    for h in order:
        picked[h] = product(sent[...], tables[h]).astype(jnp.bfloat16)
        copy = pltpu.make_async_remote_copy(
            src_ref=picked.at[h],
            dst_ref=received.at[h],
            send_sem=halo_send_sem.at[h],
            recv_sem=halo_recv_sem.at[h],
            device_id=(peer(steps[h]),),
            device_id_type=MESH,
        )
        copy.start()
        halo_copies.append(copy)
    ghosts = []
    line = jnp.zeros((1, lanes), jnp.int32)
    for h in range(len(steps)):
        for r in range(depth):
            used = (line + halo_rows[0, h]) > r
            ghosts.append(jnp.where(used, halo_ghost[0, h, r : r + 1, :], -1))
    columns = jnp.transpose(jnp.concatenate(ghosts, axis=0))
    ones = jnp.ones((16, len(ghosts) * lanes), jnp.bfloat16)

    def scatter_cells(index, _):
        base = pl.multiple_of(index * rows, rows)
        run = pl.ds(base, rows)
        ids = lax.broadcasted_iota(jnp.int32, (lanes, rows), 1) + base
        pull = 0.25 * wet[0:1, run].astype(jnp.float32)
        for i in range(len(ghosts)):
            hit = ids == columns[:, i : i + 1]
            scatter[i * lanes : (i + 1) * lanes, run] = jnp.where(hit, pull, 0.0).astype(
                jnp.bfloat16
            )
        keep = 1.0 - product(ones, scatter[:, run])[0:1]
        for t in range(tracers):
            mixed[t, :, run] = keep * mixed[t, :, run]
        return 0

    lax.fori_loop(0, cells // rows, scatter_cells, 0)
    for copy in halo_copies:
        copy.wait()


def halo_kernel(received, scatter, kept, flux_in, flux_out, out):
    tracers, levels, tile = out.shape
    run = pl.ds(pl.multiple_of(pl.program_id(0) * tile, tile), tile)
    values = jnp.concatenate([received[h] for h in range(received.shape[0])], axis=1)
    summed = product(values, scatter[:, run])
    for t in range(tracers):
        out[t] = kept[t, :, run] + summed[t * levels : (t + 1) * levels]
    flux_out[...] = flux_in[...]


def body(
    atm_flux,
    remap_send,
    remap_target,
    remap_counts,
    remap_weights,
    coupling,
    tracer,
    wet,
    mix_inverse,
    halo_send,
    halo_ghost,
    halo_rows,
):
    spans, slots = remap_send.shape[1:]
    block = remap_weights.shape[-1]
    fluxes = atm_flux.shape[0]
    tracers, levels, cells = tracer.shape
    blocks = cells // block
    hosts, depth, lanes = halo_send.shape[1:]
    picks = depth * lanes
    features = tracers * levels
    wet_row = wet.reshape(1, cells)
    vmem = pl.BlockSpec(memory_space=pltpu.VMEM)
    smem = pl.BlockSpec(memory_space=pltpu.SMEM)
    hbm = pl.BlockSpec(memory_space=pltpu.HBM)
    flux, kept, received, scatter = pl.pallas_call(
        couple_kernel,
        out_shape=(
            pltpu.VMEM((fluxes, cells), jnp.float32),
            pltpu.VMEM((tracers, levels, cells), jnp.float32),
            pltpu.VMEM((hosts, features, picks), jnp.bfloat16),
            pltpu.VMEM((hosts * picks, cells), jnp.bfloat16),
        ),
        in_specs=[smem] * 5 + [vmem] * 4 + [hbm] * 3,
        out_specs=(vmem, vmem, vmem, vmem),
        scratch_shapes=[
            pltpu.VMEM((spans, slots, block, block), jnp.bfloat16),
            pltpu.VMEM((tracers, levels, cells), jnp.float32),
            pltpu.VMEM((blocks, levels, levels), jnp.float32),
            pltpu.VMEM((features, cells), jnp.bfloat16),
            pltpu.VMEM((tracers, cells), jnp.float32),
            pltpu.VMEM((blocks * fluxes, block), jnp.float32),
            pltpu.VMEM((spans, slots, fluxes, block), jnp.bfloat16),
            pltpu.VMEM((spans, slots, fluxes, block), jnp.bfloat16),
            pltpu.VMEM((hosts, cells, picks), jnp.bfloat16),
            pltpu.VMEM((hosts, features, picks), jnp.bfloat16),
            pltpu.SemaphoreType.DMA((2 * CHUNKS + 1,)),
            pltpu.SemaphoreType.DMA((spans,)),
            pltpu.SemaphoreType.DMA((spans,)),
            pltpu.SemaphoreType.DMA((hosts,)),
            pltpu.SemaphoreType.DMA((hosts,)),
        ],
        compiler_params=pltpu.CompilerParams(
            collective_id=0, has_side_effects=True, vmem_limit_bytes=50 * 1024 * 1024 + 512 * 1024
        ),
        name="couple",
    )(
        remap_send.transpose(1, 0, 2),
        remap_target.transpose(1, 0, 2),
        remap_counts,
        coupling,
        halo_rows,
        atm_flux,
        wet_row,
        halo_send,
        halo_ghost,
        remap_weights,
        tracer,
        mix_inverse,
    )
    tile = min(TILE, cells)
    return pl.pallas_call(
        halo_kernel,
        grid=(cells // tile,),
        out_shape=(
            jax.ShapeDtypeStruct((fluxes, cells), jnp.float32),
            jax.ShapeDtypeStruct((tracers, levels, cells), jnp.float32),
        ),
        in_specs=[vmem, vmem, vmem, pl.BlockSpec((fluxes, tile), lambda i: (0, i))],
        out_specs=(
            pl.BlockSpec((fluxes, tile), lambda i: (0, i)),
            pl.BlockSpec((tracers, levels, tile), lambda i: (0, 0, i)),
        ),
        compiler_params=pltpu.CompilerParams(vmem_limit_bytes=32 * 1024 * 1024),
        name="halo",
    )(received, scatter, kept, flux)


def solution(mesh):
    return jax.shard_map(
        body,
        mesh=mesh,
        in_specs=(
            P(None, "patch"),
            P("patch", None, None),
            P("patch", None, None),
            P("patch", None),
            P("patch", None, None, None, None),
            P(),
            P(None, None, "patch"),
            P("patch"),
            P("patch", None, None),
            P("patch", None, None, None),
            P("patch", None, None, None),
            P("patch", None),
        ),
        out_specs=(P(None, "patch"), P(None, None, "patch")),
        check_vma=False,
    )
```
